32 devices in a mesh: mem: 16 (over z, y, x), rep: 2 (over core).
Axes of the slice: x: 2, y: 2, z: 4, core: 2. Of those that a mesh axis runs over, the one named last changes fastest.
Arguments:
- particle_vectors: bfloat16 [64, 131072], P('mem', 'rep'), may hold values from -6 to 6
- observed: bfloat16 [64, 131072], P('mem', 'rep'), may hold values from -24 to 24
- precision: float32 [131072], P('rep'), may hold values from 0.5 to 240, as said below
- entry_projection_matrix: bfloat16 [2, 256, 1024], replicated, may hold values from -0.375 to 0.375
- entry_offsets: float32 [2, 1024], replicated, may hold values from -3 to 3
- exit_projection_matrix: bfloat16 [2, 1024, 256], replicated, may hold values from -0.1875 to 0.1875
- exit_offsets: float32 [2, 256], replicated, may hold values from -3 to 3
Outputs:
- updated: bfloat16 [64, 131072], P('mem', 'rep')
The draws below stay inside these ranges and needn't reach their ends.
Inputs may be any that keep to these rules, and one draw needn't show every extreme that they name: `precision`: positive precisions.
All inputs are finite; a program needn't handle non-finite values.
Results may differ from the reference program's by a relative error of at most 0.0065.
Values may be sent and summed in bfloat16 or wider, within the bound.
No kernel may reach another device: no remote copies, remote signals or barrier semaphores. Data moves between devices by JAX's collectives and lax.ppermute only.
A program may use at most 64 MiB of HBM per device.

```python
import jax
import jax.numpy as jnp
from jax import lax

PW = 256
HID = 1024
LAYERS = 2
PATCHES = 512
MEMBERS = 64
STATE = 131072
BLOCK = 4096


def draw_precision(key, part):
    place = jnp.arange(STATE, dtype=jnp.float32) / STATE
    rising = jnp.exp(jnp.log(3.0) * place)
    rough = jnp.exp(jax.random.uniform(key, (STATE,), jnp.float32, jnp.log(0.5), jnp.log(2.0)))
    block_ids = jnp.arange(STATE, dtype=jnp.int32) // BLOCK
    heavy_blocks = jax.random.randint(jax.random.fold_in(key, 5), (3,), 0, STATE // BLOCK, dtype=jnp.int32)
    is_heavy = jnp.any(block_ids[:, None] == heavy_blocks[None, :], axis=1)
    boost = jnp.where(is_heavy, 40.0, 1.0).astype(jnp.float32)
    return rising * rough * boost


def draw_observed(key, part):
    local_key = jax.random.fold_in(key, 17)
    place = jnp.arange(MEMBERS, dtype=jnp.float32) / max(MEMBERS - 1, 1)
    row_scale = jnp.exp(jnp.log(4.0) * place)
    noise = jnp.clip(jax.random.normal(local_key, (MEMBERS, STATE), jnp.float32), -6.0, 6.0)
    return (noise * row_scale[:, None]).astype(jnp.bfloat16)


def levels(rng, shape, split, low, largest):
    level = 1.0
    for dim, parts in split:
        heights = jax.random.uniform(jax.random.fold_in(jax.random.fold_in(rng, 6), dim), (parts,), jnp.float32, low / len(split), largest / len(split))
        level = level * jnp.repeat(jnp.exp(heights), shape[dim] // parts).reshape((-1,) + (1,) * (len(shape) - 1 - dim))
    return level


def normal_values(own_key, shape, scale, reach, split=(), kind=jnp.bfloat16):
    entries = scale * jax.random.normal(own_key, shape, jnp.float32)
    if split:
        entries = entries * levels(own_key, shape, split, -0.22, 0.18)
    return jnp.clip(entries, -reach, reach).astype(kind)


def setup_inputs(seed: int = 0) -> dict:
    arg_keys = jax.random.split(jax.random.key(seed), 8)
    particle_vectors = normal_values(arg_keys[0], (MEMBERS, STATE), 1.0, 6.0, ((0, 16), (1, 2)))
    observed = draw_observed(jax.random.fold_in(arg_keys[7], 71), 0)
    precision = draw_precision(jax.random.fold_in(arg_keys[7], 71), 0)
    entry_projection_matrix = normal_values(arg_keys[3], (LAYERS, PW, HID), PW ** -0.5, 0.375)
    entry_offsets = normal_values(arg_keys[4], (LAYERS, HID), 0.5, 3.0, (), jnp.float32)
    exit_projection_matrix = normal_values(arg_keys[5], (LAYERS, HID, PW), HID ** -0.5, 0.1875)
    exit_offsets = normal_values(arg_keys[6], (LAYERS, PW), 0.5, 3.0, (), jnp.float32)
    return {"particle_vectors": particle_vectors, "observed": observed, "precision": precision, "entry_projection_matrix": entry_projection_matrix, "entry_offsets": entry_offsets, "exit_projection_matrix": exit_projection_matrix, "exit_offsets": exit_offsets}


def patch_network(particle_index, entry_projection_matrix, entry_offsets, exit_projection_matrix, exit_offsets):
    stream = particle_index.reshape(PATCHES, PW)
    for layer in range(LAYERS):
        pre = jnp.dot(stream.astype(jnp.float32), entry_projection_matrix[layer].astype(jnp.float32), preferred_element_type=jnp.float32) + entry_offsets[layer]
        hidden = jax.nn.silu(pre).astype(jnp.bfloat16)
        stream = (stream.astype(jnp.float32) + jnp.dot(hidden.astype(jnp.float32), exit_projection_matrix[layer].astype(jnp.float32), preferred_element_type=jnp.float32) + exit_offsets[layer]).astype(jnp.bfloat16)
    return stream.reshape(STATE)

def reference(particle_vectors, observed, precision, entry_projection_matrix, entry_offsets, exit_projection_matrix, exit_offsets):
    particle_outcomes = lax.map(lambda particle_index: patch_network(particle_index, entry_projection_matrix, entry_offsets, exit_projection_matrix, exit_offsets), particle_vectors)
    resid = (observed.astype(jnp.float32) - particle_outcomes.astype(jnp.float32)).astype(jnp.bfloat16)
    resid_wide = resid.astype(jnp.float32)
    damping = jnp.sum(resid_wide * resid_wide * precision) / (MEMBERS * STATE) + 1e-06
    pred_wide = particle_outcomes.astype(jnp.float32)
    pred_dev = (pred_wide - jnp.mean(pred_wide, axis=0)).astype(jnp.bfloat16)
    state_wide = particle_vectors.astype(jnp.float32)
    state_dev = (state_wide - jnp.mean(state_wide, axis=0)).astype(jnp.bfloat16)
    weighted = (pred_dev.astype(jnp.float32) * precision).astype(jnp.bfloat16)
    gram = jnp.dot(weighted.astype(jnp.float32), pred_dev.T.astype(jnp.float32), preferred_element_type=jnp.float32) / STATE
    cross = jnp.dot(resid.astype(jnp.float32), weighted.T.astype(jnp.float32), preferred_element_type=jnp.float32) / STATE
    kmat = gram + damping * jnp.eye(MEMBERS, dtype=jnp.float32)
    factor = jnp.linalg.cholesky(kmat)
    middle = jax.scipy.linalg.solve_triangular(factor, cross.T, lower=True)
    solved = jax.scipy.linalg.solve_triangular(factor, middle, lower=True, trans='T')
    mixing = solved.T.astype(jnp.bfloat16)
    return (state_wide + jnp.dot(mixing.astype(jnp.float32), state_dev.astype(jnp.float32), preferred_element_type=jnp.float32)).astype(jnp.bfloat16)
```

```python
import jax
import jax.numpy as jnp
from jax import lax
from jax.sharding import PartitionSpec as P

PW = 256
LAYERS = 2


def contract(left, right):
    return lax.dot_general(
        left, right, (((1,), (1,)), ((), ())), preferred_element_type=jnp.float32
    )


def to_block(value):
    return lax.all_to_all(value, "mem", split_axis=1, concat_axis=0, tiled=True)


def total_over_devices(value):
    for axis in ("rep", "mem"):
        size = lax.axis_size(axis)
        if size & (size - 1):
            value = lax.psum(value, axis)
            continue
        bit = 1
        while bit < size:
            mask = bit ^ (bit >> 1) if bit * 2 == size else bit
            value = value + lax.ppermute(value, axis, [(i, i ^ mask) for i in range(size)])
            bit *= 2
    return value


def forecast(states, entry_w, entry_b, exit_w, exit_b):
    members, width = states.shape
    stream = states.reshape(members, width // PW, PW).transpose(1, 0, 2).reshape(-1, PW)
    for layer in range(LAYERS):
        pre = jnp.dot(stream, entry_w[layer], preferred_element_type=jnp.float32) + entry_b[layer]
        hidden = jax.nn.silu(pre).astype(jnp.bfloat16)
        stream = (
            stream.astype(jnp.float32)
            + jnp.dot(hidden, exit_w[layer], preferred_element_type=jnp.float32)
            + exit_b[layer]
        ).astype(jnp.bfloat16)
    return stream.reshape(width // PW, members, PW).transpose(1, 0, 2).reshape(members, width)


def body(
    particle_vectors,
    observed,
    precision,
    entry_projection_matrix,
    entry_offsets,
    exit_projection_matrix,
    exit_offsets,
):
    state_total = particle_vectors.shape[1] * lax.axis_size("rep")
    own_states = to_block(particle_vectors)
    own_obs = to_block(observed)
    member_total, block_width = own_states.shape
    prec_block = lax.dynamic_slice_in_dim(
        precision, lax.axis_index("mem") * block_width, block_width
    )
    own_preds = forecast(
        own_states, entry_projection_matrix, entry_offsets, exit_projection_matrix, exit_offsets
    )
    pred_wide = own_preds.astype(jnp.float32)
    pred_dev = (pred_wide - jnp.mean(pred_wide, axis=0)).astype(jnp.bfloat16)
    weighted = (pred_dev.astype(jnp.float32) * prec_block).astype(jnp.bfloat16)
    state_wide = own_states.astype(jnp.float32)
    state_dev = (state_wide - jnp.mean(state_wide, axis=0)).astype(jnp.bfloat16)
    gram = contract(weighted, pred_dev)
    resid = (own_obs.astype(jnp.float32) - pred_wide).astype(jnp.bfloat16)
    resid_wide = resid.astype(jnp.float32)
    misfit = jnp.sum(resid_wide * resid_wide * prec_block)
    cross_t = contract(weighted, resid)
    eye = jnp.eye(member_total, dtype=jnp.float32)
    joined = jnp.concatenate([gram + (misfit / member_total) * eye, cross_t], axis=1)
    joined = total_over_devices(joined) / state_total
    kmat = joined[:, :member_total] + 1e-06 * eye
    factor = jnp.linalg.cholesky(kmat)
    middle = jax.scipy.linalg.solve_triangular(factor, joined[:, member_total:], lower=True)
    solved = jax.scipy.linalg.solve_triangular(factor, middle, lower=True, trans="T")
    mixing = solved.T.astype(jnp.bfloat16)
    fresh = (
        state_wide + jnp.dot(mixing, state_dev, preferred_element_type=jnp.float32)
    ).astype(jnp.bfloat16)
    return lax.all_to_all(fresh, "mem", split_axis=0, concat_axis=1, tiled=True)


def solution(mesh):
    placed = (P("mem", "rep"), P("mem", "rep"), P("rep"), P(), P(), P(), P())
    return jax.shard_map(
        body, mesh=mesh, in_specs=placed, out_specs=P("mem", "rep"), check_vma=False
    )
```

```python
import jax
import jax.numpy as jnp
from jax import lax
from jax.experimental import pallas as pl
from jax.experimental.pallas import tpu as pltpu
from jax.sharding import PartitionSpec as P

PW = 256
LAYERS = 2
SUB = 8
LANES = 128
CHUNK = 512
VMEM_LIMIT = 8 * 1024 * 1024


def contract(left, right):
    return lax.dot_general(
        left, right, (((1,), (1,)), ((), ())), preferred_element_type=jnp.float32
    )


def to_block(value):
    return lax.all_to_all(value, "mem", split_axis=1, concat_axis=0, tiled=True)


def total_over_devices(value):
    other = jnp.zeros_like(value)
    for axis in ("rep", "mem"):
        size = lax.axis_size(axis)
        if size & (size - 1):
            value, other = lax.psum(value + other, axis), jnp.zeros_like(value)
            continue
        bit = 1
        while bit < size:
            mask = bit ^ (bit >> 1) if bit * 2 == size else bit
            value = value + other
            other = lax.ppermute(value, axis, [(i, i ^ mask) for i in range(size)])
            bit *= 2
    return value, other


def forecast(states, entry_w, entry_b, exit_w, exit_b):
    members, width = states.shape
    stream = states.reshape(members, width // PW, PW).transpose(1, 0, 2).reshape(-1, PW)
    for layer in range(LAYERS):
        pre = jnp.dot(stream, entry_w[layer], preferred_element_type=jnp.float32) + entry_b[layer]
        hidden = jax.nn.silu(pre).astype(jnp.bfloat16)
        stream = (
            stream.astype(jnp.float32)
            + jnp.dot(hidden, exit_w[layer], preferred_element_type=jnp.float32)
            + exit_b[layer]
        ).astype(jnp.bfloat16)
    return stream.reshape(width // PW, members, PW).transpose(1, 0, 2).reshape(members, width)


def eliminate(blocks, first):
    shape = blocks[0].shape
    row = lax.broadcasted_iota(jnp.int32, shape, 0)
    for kb in range(len(blocks)):
        lo = first + kb * SUB
        cols = [
            [jnp.broadcast_to(block[:, lo + j : lo + j + 1], shape) for j in range(SUB)]
            for block in blocks
        ]
        pivot = blocks[kb]
        own = list(cols[kb])
        for p in range(SUB):
            factor = own[p]
            inv = 1.0 / factor[p : p + 1, :]
            line = pivot[p : p + 1, :] * inv
            pivot = jnp.where(row == p, line, pivot - factor * line)
            for j in range(p + 1, SUB):
                line = own[j][p : p + 1, :] * inv
                own[j] = jnp.where(row == p, line, own[j] - factor * line)
        after = []
        for i, block in enumerate(blocks):
            if i == kb:
                after.append(pivot)
                continue
            terms = [cols[i][j] * pivot[j : j + 1, :] for j in range(SUB)]
            while len(terms) > 1:
                terms = [terms[t] + terms[t + 1] for t in range(0, len(terms), 2)]
            after.append(block - terms[0])
        blocks = after
    return blocks


def finish_kernel(scale, shift, mine_ref, other_ref, states_ref, dev_ref, out_ref):
    members, width = states_ref.shape
    row = lax.broadcasted_iota(jnp.int32, (SUB, 2 * members), 0)
    lane = lax.broadcasted_iota(jnp.int32, (SUB, 2 * members), 1)
    blocks = []
    for lo in range(0, members, SUB):
        rows = slice(lo, lo + SUB)
        block = (mine_ref[rows, :] + other_ref[rows, :]) * scale
        blocks.append(block + jnp.where(lane == row + (members + lo), shift, 0.0))
    solved = jnp.concatenate([b[:, :members] for b in eliminate(blocks, members)], axis=0)
    mixing = solved.T.astype(jnp.bfloat16)
    step = min(CHUNK, width)
    for lo in range(0, width, step):
        cols = slice(lo, lo + step)
        move = jnp.dot(mixing, dev_ref[:, cols], preferred_element_type=jnp.float32)
        out_ref[:, cols] = (states_ref[:, cols].astype(jnp.float32) + move).astype(jnp.bfloat16)


def finish(scale, shift, mine, other, states, dev):
    vmem = pl.BlockSpec(memory_space=pltpu.VMEM)
    return pl.pallas_call(
        lambda *refs: finish_kernel(scale, shift, *refs),
        out_shape=jax.ShapeDtypeStruct(states.shape, jnp.bfloat16),
        in_specs=[vmem] * 4,
        out_specs=vmem,
        compiler_params=pltpu.CompilerParams(vmem_limit_bytes=VMEM_LIMIT),
        name="finish",
    )(mine, other, states, dev)


def finish_plain(scale, shift, mine, other, states, dev):
    members = states.shape[0]
    joined = (mine + other) * scale
    kmat = joined[:, members:] + shift * jnp.eye(members, dtype=jnp.float32)
    factor = jnp.linalg.cholesky(kmat)
    middle = jax.scipy.linalg.solve_triangular(factor, joined[:, :members], lower=True)
    solved = jax.scipy.linalg.solve_triangular(factor, middle, lower=True, trans="T")
    mixing = solved.T.astype(jnp.bfloat16)
    return (
        states.astype(jnp.float32) + jnp.dot(mixing, dev, preferred_element_type=jnp.float32)
    ).astype(jnp.bfloat16)


def body(
    particle_vectors,
    observed,
    precision,
    entry_projection_matrix,
    entry_offsets,
    exit_projection_matrix,
    exit_offsets,
):
    state_total = particle_vectors.shape[1] * lax.axis_size("rep")
    own_states = to_block(particle_vectors)
    own_obs = to_block(observed)
    member_total, block_width = own_states.shape
    prec_block = lax.dynamic_slice_in_dim(
        precision, lax.axis_index("mem") * block_width, block_width
    )
    own_preds = forecast(
        own_states, entry_projection_matrix, entry_offsets, exit_projection_matrix, exit_offsets
    )
    pred_wide = own_preds.astype(jnp.float32)
    pred_dev = (pred_wide - jnp.mean(pred_wide, axis=0)).astype(jnp.bfloat16)
    weighted = (pred_dev.astype(jnp.float32) * prec_block).astype(jnp.bfloat16)
    state_wide = own_states.astype(jnp.float32)
    state_dev = (state_wide - jnp.mean(state_wide, axis=0)).astype(jnp.bfloat16)
    gram = contract(weighted, pred_dev)
    resid = (own_obs.astype(jnp.float32) - pred_wide).astype(jnp.bfloat16)
    resid_wide = resid.astype(jnp.float32)
    misfit = jnp.sum(resid_wide * resid_wide * prec_block)
    cross_t = contract(weighted, resid)
    eye = jnp.eye(member_total, dtype=jnp.float32)
    gram = 0.5 * (gram + gram.T)
    joined = jnp.concatenate([cross_t, gram + (misfit / member_total) * eye], axis=1)
    mine, other = total_over_devices(joined)
    last = finish if member_total <= LANES // 2 and member_total % SUB == 0 else finish_plain
    fresh = last(1.0 / state_total, 1e-06, mine, other, own_states, state_dev)
    return lax.all_to_all(fresh, "mem", split_axis=0, concat_axis=1, tiled=True)


def solution(mesh):
    placed = (P("mem", "rep"), P("mem", "rep"), P("rep"), P(), P(), P(), P())
    return jax.shard_map(
        body, mesh=mesh, in_specs=placed, out_specs=P("mem", "rep"), check_vma=False
    )
```

```python
import jax
import jax.numpy as jnp
from jax import lax
from jax.experimental import pallas as pl
from jax.experimental.pallas import tpu as pltpu
from jax.sharding import PartitionSpec as P

PW = 256
LAYERS = 2
SUB = 8
LANES = 128
CHUNK = 512
VMEM_LIMIT = 8 * 1024 * 1024


def contract(left, right):
    return lax.dot_general(
        left, right, (((1,), (1,)), ((), ())), preferred_element_type=jnp.float32
    )


def halves(count):
    half = count // 2
    return [list(range(half)), [half + (i ^ (half // 2)) for i in range(half)]]


def to_block(value, groups):
    rows, _ = value.shape
    return lax.all_to_all(
        value.reshape(rows, len(groups[0]), -1),
        "mem", split_axis=1, concat_axis=0, axis_index_groups=groups,
    )


def mirror(value, groups):
    pairs = list(zip(*groups))
    return lax.ppermute(value, "mem", pairs + [(b, a) for a, b in pairs])


def total_over_half(value):
    count = lax.axis_size("mem")
    steps = [("rep", 2, 1)]
    bit = 1
    while bit < count // 2:
        steps.append(("mem", count, bit))
        bit *= 2
    other = jnp.zeros_like(value)
    for axis, size, mask in steps:
        value = value + other
        other = lax.ppermute(value, axis, [(i, i ^ mask) for i in range(size)])
    return value, other


def by_patch(value):
    rows, width = value.shape
    return value.reshape(rows, width // PW, PW).transpose(1, 0, 2).reshape(-1, PW)


def forecast_block(stream, layer, entry_w, entry_b, exit_w, exit_b):
    pre = jnp.dot(stream, entry_w[layer], preferred_element_type=jnp.float32) + entry_b[layer]
    hidden = jax.nn.silu(pre).astype(jnp.bfloat16)
    return (
        stream.astype(jnp.float32)
        + jnp.dot(hidden, exit_w[layer], preferred_element_type=jnp.float32)
        + exit_b[layer]
    ).astype(jnp.bfloat16)


def residual_kernel(obs_ref, own_ref, prec_ref, resid_ref, misfit_ref):
    patches = prec_ref.shape[0]
    rows = own_ref.shape[0] // patches
    total = jnp.zeros((rows, PW), jnp.float32)
    for p in range(patches):
        part = slice(p * rows, (p + 1) * rows)
        resid = (
            obs_ref[part, :].astype(jnp.float32) - own_ref[part, :].astype(jnp.float32)
        ).astype(jnp.bfloat16)
        resid_ref[part, :] = resid
        wide = resid.astype(jnp.float32)
        total = total + wide * wide * prec_ref[p : p + 1, :]
    misfit_ref[...] = jnp.full(misfit_ref.shape, jnp.sum(total))


def residual(obs, own, prec):
    vmem = pl.BlockSpec(memory_space=pltpu.VMEM)
    return pl.pallas_call(
        residual_kernel,
        out_shape=(
            jax.ShapeDtypeStruct(own.shape, jnp.bfloat16),
            jax.ShapeDtypeStruct((SUB, LANES), jnp.float32),
        ),
        in_specs=[vmem] * 3,
        out_specs=(vmem, vmem),
        compiler_params=pltpu.CompilerParams(vmem_limit_bytes=VMEM_LIMIT),
        name="residual",
    )(obs, own, prec)


def terms_kernel(own_ref, far_ref, resid_ref, prec_ref, share_ref, out_ref):
    patches = prec_ref.shape[0]
    rows = own_ref.shape[0] // patches
    members = 2 * rows
    cross = jnp.zeros((members, rows), jnp.float32)
    gram = jnp.zeros((members, members), jnp.float32)
    for p in range(patches):
        part = slice(p * rows, (p + 1) * rows)
        own = own_ref[part, :].astype(jnp.float32)
        far = far_ref[part, :].astype(jnp.float32)
        mean = (jnp.sum(own, axis=0, keepdims=True) + jnp.sum(far, axis=0, keepdims=True)) * (
            1.0 / members
        )
        dev = jnp.concatenate([own - mean, far - mean], axis=0).astype(jnp.bfloat16)
        weighted = (dev.astype(jnp.float32) * prec_ref[p : p + 1, :]).astype(jnp.bfloat16)
        cross = cross + contract(weighted, resid_ref[part, :])
        gram = gram + contract(weighted, dev)
    gram = 0.5 * (gram + gram.T)
    row = lax.broadcasted_iota(jnp.int32, (members, members), 0)
    col = lax.broadcasted_iota(jnp.int32, (members, members), 1)
    gram = gram + jnp.where(row == col, share_ref[0:1, 0:1], 0.0)
    out_ref[...] = jnp.concatenate([cross, jnp.zeros_like(cross), gram], axis=1)


def terms(own, far, resid, prec, share):
    patches = prec.shape[0]
    members = 2 * own.shape[0] // patches
    vmem = pl.BlockSpec(memory_space=pltpu.VMEM)
    return pl.pallas_call(
        terms_kernel,
        out_shape=jax.ShapeDtypeStruct((members, 2 * members), jnp.float32),
        in_specs=[vmem] * 5,
        out_specs=vmem,
        compiler_params=pltpu.CompilerParams(vmem_limit_bytes=VMEM_LIMIT),
        name="terms",
    )(own, far, resid, prec, share)


def terms_plain(own, far, resid, prec, share):
    patches = prec.shape[0]
    rows = own.shape[0] // patches
    members = 2 * rows

    def by_member(value):
        return value.reshape(patches, rows, PW).transpose(1, 0, 2).reshape(rows, patches * PW)

    preds = jnp.concatenate([by_member(own), by_member(far)], axis=0).astype(jnp.float32)
    dev = (preds - jnp.mean(preds, axis=0)).astype(jnp.bfloat16)
    weighted = (dev.astype(jnp.float32) * prec.reshape(-1)).astype(jnp.bfloat16)
    cross = contract(weighted, by_member(resid))
    gram = contract(weighted, dev)
    gram = 0.5 * (gram + gram.T) + share[0, 0] * jnp.eye(members, dtype=jnp.float32)
    return jnp.concatenate([cross, jnp.zeros_like(cross), gram], axis=1)


def eliminate(blocks, first):
    shape = blocks[0].shape
    row = lax.broadcasted_iota(jnp.int32, shape, 0)
    for kb in range(len(blocks)):
        lo = first + kb * SUB
        cols = [
            [jnp.broadcast_to(block[:, lo + j : lo + j + 1], shape) for j in range(SUB)]
            for block in blocks
        ]
        pivot = blocks[kb]
        own = list(cols[kb])
        for p in range(SUB):
            factor = own[p]
            inv = 1.0 / factor[p : p + 1, :]
            line = pivot[p : p + 1, :] * inv
            pivot = jnp.where(row == p, line, pivot - factor * line)
            for j in range(p + 1, SUB):
                line = own[j][p : p + 1, :] * inv
                own[j] = jnp.where(row == p, line, own[j] - factor * line)
        after = []
        for i, block in enumerate(blocks):
            if i == kb:
                after.append(pivot)
                continue
            terms = [cols[i][j] * pivot[j : j + 1, :] for j in range(SUB)]
            while len(terms) > 1:
                terms = [terms[t] + terms[t + 1] for t in range(0, len(terms), 2)]
            after.append(block - terms[0])
        blocks = after
    return blocks


def finish_kernel(scale, shift, mine_ref, other_ref, states_ref, dev_ref, out_ref):
    rows, width = states_ref.shape
    members = dev_ref.shape[0]
    row = lax.broadcasted_iota(jnp.int32, (SUB, 2 * members), 0)
    lane = lax.broadcasted_iota(jnp.int32, (SUB, 2 * members), 1)
    blocks = []
    for lo in range(0, members, SUB):
        part = slice(lo, lo + SUB)
        block = (mine_ref[part, :] + other_ref[part, :]) * scale
        blocks.append(block + jnp.where(lane == row + (members + lo), shift, 0.0))
    solved = jnp.concatenate([b[:, :members] for b in eliminate(blocks, members)], axis=0)
    mixing = solved.T[:rows, :].astype(jnp.bfloat16)
    step = min(CHUNK, width)
    for lo in range(0, width, step):
        cols = slice(lo, lo + step)
        move = jnp.dot(mixing, dev_ref[:, cols], preferred_element_type=jnp.float32)
        out_ref[:, cols] = (states_ref[:, cols].astype(jnp.float32) + move).astype(jnp.bfloat16)


def finish(scale, shift, mine, other, states, dev):
    vmem = pl.BlockSpec(memory_space=pltpu.VMEM)
    return pl.pallas_call(
        lambda *refs: finish_kernel(scale, shift, *refs),
        out_shape=jax.ShapeDtypeStruct(states.shape, jnp.bfloat16),
        in_specs=[vmem] * 4,
        out_specs=vmem,
        compiler_params=pltpu.CompilerParams(vmem_limit_bytes=VMEM_LIMIT),
        name="finish",
    )(mine, other, states, dev)


def finish_plain(scale, shift, mine, other, states, dev):
    rows, members = states.shape[0], dev.shape[0]
    joined = (mine + other) * scale
    kmat = joined[:, members:] + shift * jnp.eye(members, dtype=jnp.float32)
    factor = jnp.linalg.cholesky(kmat)
    middle = jax.scipy.linalg.solve_triangular(factor, joined[:, :rows], lower=True)
    solved = jax.scipy.linalg.solve_triangular(factor, middle, lower=True, trans="T")
    mixing = solved.T.astype(jnp.bfloat16)
    return (
        states.astype(jnp.float32) + jnp.dot(mixing, dev, preferred_element_type=jnp.float32)
    ).astype(jnp.bfloat16)


def body(
    particle_vectors,
    observed,
    precision,
    entry_projection_matrix,
    entry_offsets,
    exit_projection_matrix,
    exit_offsets,
):
    weights = (entry_projection_matrix, entry_offsets, exit_projection_matrix, exit_offsets)
    count = lax.axis_size("mem")
    if lax.axis_size("rep") != 2 or count < 4 or count & (count - 1):
        raise ValueError("unsupported mesh")
    groups = halves(count)
    state_total = particle_vectors.shape[1] * lax.axis_size("rep")
    member_total = particle_vectors.shape[0] * count
    own_states = to_block(particle_vectors, groups)
    far_states = mirror(own_states, groups)
    own_obs = to_block(observed, groups)
    width = own_states.shape[-1]
    own_states, far_states, own_obs = (
        v.reshape(-1, width) for v in (own_states, far_states, own_obs)
    )
    me = lax.axis_index("mem")
    place = jnp.where(me < count // 2, me, jnp.bitwise_xor(me - count // 2, count // 4))
    prec_block = lax.dynamic_slice_in_dim(precision, place * width, width).reshape(-1, PW)

    own_preds = by_patch(own_states)
    for layer in range(LAYERS):
        own_preds = forecast_block(own_preds, layer, *weights)
    resid, misfit = residual(by_patch(own_obs), own_preds, prec_block)
    far_preds = by_patch(far_states)
    for layer in range(LAYERS):
        far_preds = forecast_block(far_preds, layer, *weights)
        if layer == 0:
            far_preds, misfit = lax.optimization_barrier((far_preds, misfit))
    share = (misfit + mirror(misfit, groups)) * (1.0 / member_total)

    small = member_total <= LANES // 2 and member_total % (2 * SUB) == 0
    joined = (terms if small else terms_plain)(own_preds, far_preds, resid, prec_block, share)
    mine, other = total_over_half(joined)

    states = jnp.concatenate([own_states, far_states], axis=0).astype(jnp.float32)
    dev = (states - jnp.mean(states, axis=0)).astype(jnp.bfloat16)
    fresh = (finish if small else finish_plain)(
        1.0 / state_total, 1e-06, mine, other, own_states, dev
    )
    return lax.all_to_all(
        fresh, "mem", split_axis=0, concat_axis=1, tiled=True, axis_index_groups=groups
    )


def solution(mesh):
    placed = (P("mem", "rep"), P("mem", "rep"), P("rep"), P(), P(), P(), P())
    return jax.shard_map(
        body, mesh=mesh, in_specs=placed, out_specs=P("mem", "rep"), check_vma=False
    )
```

```python
import jax
import jax.numpy as jnp
from jax import lax
from jax.experimental import pallas as pl
from jax.experimental.pallas import tpu as pltpu
from jax.sharding import PartitionSpec as P

PW = 256
SUB = 8
LANES = 128
CHUNK = 512
ROWS = 512
VMEM_LIMIT = 8 * 1024 * 1024


def contract(left, right):
    return lax.dot_general(
        left, right, (((1,), (1,)), ((), ())), preferred_element_type=jnp.float32
    )


def halves(count):
    half = count // 2
    return [list(range(half)), [half + (i ^ (half // 2)) for i in range(half)]]


def to_block(value, groups):
    rows, _ = value.shape
    return lax.all_to_all(
        value.reshape(rows, len(groups[0]), -1),
        "mem", split_axis=1, concat_axis=0, axis_index_groups=groups,
    )


def mirror(value, groups):
    pairs = list(zip(*groups))
    return lax.ppermute(value, "mem", pairs + [(b, a) for a, b in pairs])


def total_over_half(value):
    count = lax.axis_size("mem")
    steps = [("rep", 2, 1)]
    bit = 1
    while bit < count // 2:
        steps.append(("mem", count, bit))
        bit *= 2
    other = jnp.zeros_like(value)
    for axis, size, mask in steps:
        value = value + other
        other = lax.ppermute(value, axis, [(i, i ^ mask) for i in range(size)])
    return value, other


def rows_of(ref, at):
    cols = slice(at, at + PW)
    return jnp.concatenate(
        [ref[s, :, cols].astype(jnp.float32) for s in range(ref.shape[0])], axis=0
    )


def forecast_kernel(x_ref, entry_ref, entry_b_ref, exit_ref, exit_b_ref, out_ref):
    senders, few, width = x_ref.shape
    rows = senders * few
    layers, _, hid = entry_ref.shape
    wide = min(ROWS, hid)
    each = PW * max(1, ROWS // rows)
    for first in range(0, width, each):
        starts = range(first, min(first + each, width), PW)
        stream = jnp.concatenate([rows_of(x_ref, at) for at in starts], axis=0)
        stream = stream.astype(jnp.bfloat16)
        for layer in range(layers):
            acc = stream.astype(jnp.float32) + exit_b_ref[layer : layer + 1, :]
            for at in range(0, hid, wide):
                cols = slice(at, at + wide)
                pre = jnp.dot(stream, entry_ref[layer, :, cols], preferred_element_type=jnp.float32)
                pre = pre + entry_b_ref[layer : layer + 1, cols]
                hidden = (pre * (0.5 * jnp.tanh(0.5 * pre) + 0.5)).astype(jnp.bfloat16)
                acc = acc + jnp.dot(
                    hidden, exit_ref[layer, cols, :], preferred_element_type=jnp.float32
                )
            stream = acc.astype(jnp.bfloat16)
        lo = first // PW * rows
        out_ref[lo : lo + stream.shape[0], :] = stream


def forecast(stream, entry_w, entry_b, exit_w, exit_b):
    vmem = pl.BlockSpec(memory_space=pltpu.VMEM)
    work = stream.size // PW * entry_w.size
    return pl.pallas_call(
        forecast_kernel,
        out_shape=jax.ShapeDtypeStruct((stream.size // PW, PW), jnp.bfloat16),
        in_specs=[vmem] * 5,
        out_specs=vmem,
        cost_estimate=pl.CostEstimate(
            flops=4 * work,
            bytes_accessed=4 * (stream.size + entry_w.size),
            transcendentals=work // PW,
        ),
        compiler_params=pltpu.CompilerParams(vmem_limit_bytes=2 * VMEM_LIMIT),
        name="forecast",
    )(stream, entry_w, entry_b, exit_w, exit_b)


def residual_kernel(obs_ref, own_ref, prec_ref, resid_ref, misfit_ref):
    patches = prec_ref.shape[0]
    rows = own_ref.shape[0] // patches
    total = jnp.zeros((rows, PW), jnp.float32)
    for p in range(patches):
        part = slice(p * rows, (p + 1) * rows)
        resid = (
            rows_of(obs_ref, p * PW) - own_ref[part, :].astype(jnp.float32)
        ).astype(jnp.bfloat16)
        resid_ref[part, :] = resid
        wide = resid.astype(jnp.float32)
        total = total + wide * wide * prec_ref[p : p + 1, :]
    misfit_ref[...] = jnp.full(misfit_ref.shape, jnp.sum(total))


def residual(obs, own, prec):
    vmem = pl.BlockSpec(memory_space=pltpu.VMEM)
    return pl.pallas_call(
        residual_kernel,
        out_shape=(
            jax.ShapeDtypeStruct(own.shape, jnp.bfloat16),
            jax.ShapeDtypeStruct((SUB, LANES), jnp.float32),
        ),
        in_specs=[vmem] * 3,
        out_specs=(vmem, vmem),
        compiler_params=pltpu.CompilerParams(vmem_limit_bytes=VMEM_LIMIT),
        name="residual",
    )(obs, own, prec)


def terms_kernel(own_ref, far_ref, resid_ref, prec_ref, share_ref, out_ref):
    patches = prec_ref.shape[0]
    rows = own_ref.shape[0] // patches
    members = 2 * rows
    cross = jnp.zeros((members, rows), jnp.float32)
    gram = jnp.zeros((members, members), jnp.float32)
    for p in range(patches):
        part = slice(p * rows, (p + 1) * rows)
        own = own_ref[part, :].astype(jnp.float32)
        far = far_ref[part, :].astype(jnp.float32)
        mean = (jnp.sum(own, axis=0, keepdims=True) + jnp.sum(far, axis=0, keepdims=True)) * (
            1.0 / members
        )
        dev = jnp.concatenate([own - mean, far - mean], axis=0).astype(jnp.bfloat16)
        weighted = (dev.astype(jnp.float32) * prec_ref[p : p + 1, :]).astype(jnp.bfloat16)
        cross = cross + contract(weighted, resid_ref[part, :])
        gram = gram + contract(weighted, dev)
    gram = 0.5 * (gram + gram.T)
    row = lax.broadcasted_iota(jnp.int32, (members, members), 0)
    col = lax.broadcasted_iota(jnp.int32, (members, members), 1)
    gram = gram + jnp.where(row == col, share_ref[0:1, 0:1], 0.0)
    out_ref[...] = jnp.concatenate([cross, jnp.zeros_like(cross), gram], axis=1)


def terms(own, far, resid, prec, share):
    patches = prec.shape[0]
    members = 2 * own.shape[0] // patches
    vmem = pl.BlockSpec(memory_space=pltpu.VMEM)
    return pl.pallas_call(
        terms_kernel,
        out_shape=jax.ShapeDtypeStruct((members, 2 * members), jnp.float32),
        in_specs=[vmem] * 5,
        out_specs=vmem,
        compiler_params=pltpu.CompilerParams(vmem_limit_bytes=VMEM_LIMIT),
        name="terms",
    )(own, far, resid, prec, share)


def terms_plain(own, far, resid, prec, share):
    patches = prec.shape[0]
    rows = own.shape[0] // patches
    members = 2 * rows

    def by_member(value):
        return value.reshape(patches, rows, PW).transpose(1, 0, 2).reshape(rows, patches * PW)

    preds = jnp.concatenate([by_member(own), by_member(far)], axis=0).astype(jnp.float32)
    dev = (preds - jnp.mean(preds, axis=0)).astype(jnp.bfloat16)
    weighted = (dev.astype(jnp.float32) * prec.reshape(-1)).astype(jnp.bfloat16)
    cross = contract(weighted, by_member(resid))
    gram = contract(weighted, dev)
    gram = 0.5 * (gram + gram.T) + share[0, 0] * jnp.eye(members, dtype=jnp.float32)
    return jnp.concatenate([cross, jnp.zeros_like(cross), gram], axis=1)


def eliminate(blocks, first):
    shape = blocks[0].shape
    row = lax.broadcasted_iota(jnp.int32, shape, 0)
    for kb in range(len(blocks)):
        lo = first + kb * SUB
        cols = [
            [jnp.broadcast_to(block[:, lo + j : lo + j + 1], shape) for j in range(SUB)]
            for block in blocks
        ]
        pivot = blocks[kb]
        own = list(cols[kb])
        for p in range(SUB):
            factor = own[p]
            inv = 1.0 / factor[p : p + 1, :]
            line = pivot[p : p + 1, :] * inv
            pivot = jnp.where(row == p, line, pivot - factor * line)
            for j in range(p + 1, SUB):
                line = own[j][p : p + 1, :] * inv
                own[j] = jnp.where(row == p, line, own[j] - factor * line)
        after = []
        for i, block in enumerate(blocks):
            if i == kb:
                after.append(pivot)
                continue
            terms = [cols[i][j] * pivot[j : j + 1, :] for j in range(SUB)]
            while len(terms) > 1:
                terms = [terms[t] + terms[t + 1] for t in range(0, len(terms), 2)]
            after.append(block - terms[0])
        blocks = after
    return blocks


def finish_kernel(scale, shift, mine_ref, other_ref, states_ref, dev_ref, out_ref):
    rows, width = states_ref.shape
    members = dev_ref.shape[0]
    row = lax.broadcasted_iota(jnp.int32, (SUB, 2 * members), 0)
    lane = lax.broadcasted_iota(jnp.int32, (SUB, 2 * members), 1)
    blocks = []
    for lo in range(0, members, SUB):
        part = slice(lo, lo + SUB)
        block = (mine_ref[part, :] + other_ref[part, :]) * scale
        blocks.append(block + jnp.where(lane == row + (members + lo), shift, 0.0))
    solved = jnp.concatenate([b[:, :members] for b in eliminate(blocks, members)], axis=0)
    mixing = solved.T[:rows, :].astype(jnp.bfloat16)
    step = min(CHUNK, width)
    for lo in range(0, width, step):
        cols = slice(lo, lo + step)
        move = jnp.dot(mixing, dev_ref[:, cols], preferred_element_type=jnp.float32)
        out_ref[:, cols] = (states_ref[:, cols].astype(jnp.float32) + move).astype(jnp.bfloat16)


def finish(scale, shift, mine, other, states, dev):
    vmem = pl.BlockSpec(memory_space=pltpu.VMEM)
    return pl.pallas_call(
        lambda *refs: finish_kernel(scale, shift, *refs),
        out_shape=jax.ShapeDtypeStruct(states.shape, jnp.bfloat16),
        in_specs=[vmem] * 4,
        out_specs=vmem,
        compiler_params=pltpu.CompilerParams(vmem_limit_bytes=VMEM_LIMIT),
        name="finish",
    )(mine, other, states, dev)


def finish_plain(scale, shift, mine, other, states, dev):
    rows, members = states.shape[0], dev.shape[0]
    joined = (mine + other) * scale
    kmat = joined[:, members:] + shift * jnp.eye(members, dtype=jnp.float32)
    factor = jnp.linalg.cholesky(kmat)
    middle = jax.scipy.linalg.solve_triangular(factor, joined[:, :rows], lower=True)
    solved = jax.scipy.linalg.solve_triangular(factor, middle, lower=True, trans="T")
    mixing = solved.T.astype(jnp.bfloat16)
    return (
        states.astype(jnp.float32) + jnp.dot(mixing, dev, preferred_element_type=jnp.float32)
    ).astype(jnp.bfloat16)


def body(
    particle_vectors,
    observed,
    precision,
    entry_projection_matrix,
    entry_offsets,
    exit_projection_matrix,
    exit_offsets,
):
    weights = (entry_projection_matrix, entry_offsets, exit_projection_matrix, exit_offsets)
    count = lax.axis_size("mem")
    if lax.axis_size("rep") != 2 or count < 4 or count & (count - 1):
        raise ValueError("unsupported mesh")
    groups = halves(count)
    state_total = particle_vectors.shape[1] * lax.axis_size("rep")
    member_total = particle_vectors.shape[0] * count
    own_states = to_block(particle_vectors, groups)
    far_states = mirror(own_states, groups)
    own_obs = to_block(observed, groups)
    width = own_states.shape[-1]
    rows = member_total // 2
    me = lax.axis_index("mem")
    place = jnp.where(me < count // 2, me, jnp.bitwise_xor(me - count // 2, count // 4))
    prec_block = lax.dynamic_slice_in_dim(precision, place * width, width).reshape(-1, PW)

    own_preds = forecast(own_states, *weights)
    resid, misfit = residual(own_obs, own_preds, prec_block)
    far_misfit = mirror(misfit, groups)
    far_preds = forecast(far_states, *weights)
    share = (misfit + far_misfit) * (1.0 / member_total)

    small = member_total <= LANES // 2 and member_total % (2 * SUB) == 0
    joined = (terms if small else terms_plain)(own_preds, far_preds, resid, prec_block, share)
    mine, other = total_over_half(joined)

    own_states = own_states.reshape(rows, width)
    far_states = far_states.reshape(rows, width)
    states = jnp.concatenate([own_states, far_states], axis=0).astype(jnp.float32)
    dev = (states - jnp.mean(states, axis=0)).astype(jnp.bfloat16)
    fresh = (finish if small else finish_plain)(
        1.0 / state_total, 1e-06, mine, other, own_states, dev
    )
    return lax.all_to_all(
        fresh, "mem", split_axis=0, concat_axis=1, tiled=True, axis_index_groups=groups
    )


def solution(mesh):
    placed = (P("mem", "rep"), P("mem", "rep"), P("rep"), P(), P(), P(), P())
    return jax.shard_map(
        body, mesh=mesh, in_specs=placed, out_specs=P("mem", "rep"), check_vma=False
    )
```

```python
import jax
import jax.numpy as jnp
from jax import lax
from jax.experimental import pallas as pl
from jax.experimental.pallas import tpu as pltpu
from jax.sharding import PartitionSpec as P

PW = 256
SUB = 8
LANES = 128
CHUNK = 512
ROWS = 1024
VMEM_LIMIT = 8 * 1024 * 1024


def contract(left, right):
    return lax.dot_general(
        left, right, (((1,), (1,)), ((), ())), preferred_element_type=jnp.float32
    )


def halves(count):
    half = count // 2
    return [list(range(half)), [half + (i ^ (half // 2)) for i in range(half)]]


def to_block(value, groups):
    rows, _ = value.shape
    return lax.all_to_all(
        value.reshape(rows, len(groups[0]), -1),
        "mem", split_axis=1, concat_axis=0, axis_index_groups=groups,
    )


def mirror(value, groups):
    pairs = list(zip(*groups))
    return lax.ppermute(value, "mem", pairs + [(b, a) for a, b in pairs])


def total_over_half(value):
    count = lax.axis_size("mem")
    steps = [("rep", 2, 1)]
    bit = 1
    while bit < count // 2:
        steps.append(("mem", count, bit))
        bit *= 2
    other = jnp.zeros_like(value)
    for axis, size, mask in steps:
        value = value + other
        other = lax.ppermute(value, axis, [(i, i ^ mask) for i in range(size)])
    return value, other


def rows_of(ref, at):
    cols = slice(at, at + PW)
    return jnp.concatenate(
        [ref[s, :, cols].astype(jnp.float32) for s in range(ref.shape[0])], axis=0
    )


def forecast_kernel(x_ref, entry_ref, entry_b_ref, exit_ref, exit_b_ref, out_ref):
    senders, few, width = x_ref.shape
    rows = senders * few
    layers, _, hid = entry_ref.shape
    wide = min(ROWS, hid)
    each = PW * max(1, ROWS // rows)
    for first in range(0, width, each):
        starts = range(first, min(first + each, width), PW)
        stream = jnp.concatenate([rows_of(x_ref, at) for at in starts], axis=0)
        stream = stream.astype(jnp.bfloat16)
        for layer in range(layers):
            acc = stream.astype(jnp.float32) + exit_b_ref[layer : layer + 1, :]
            for at in range(0, hid, wide):
                cols = slice(at, at + wide)
                pre = jnp.dot(stream, entry_ref[layer, :, cols], preferred_element_type=jnp.float32)
                pre = pre + entry_b_ref[layer : layer + 1, cols]
                hidden = (pre * (0.5 * jnp.tanh(0.5 * pre) + 0.5)).astype(jnp.bfloat16)
                acc = acc + jnp.dot(
                    hidden, exit_ref[layer, cols, :], preferred_element_type=jnp.float32
                )
            stream = acc.astype(jnp.bfloat16)
        lo = first // PW * rows
        out_ref[lo : lo + stream.shape[0], :] = stream


def forecast(stream, entry_w, entry_b, exit_w, exit_b):
    vmem = pl.BlockSpec(memory_space=pltpu.VMEM)
    work = stream.size // PW * entry_w.size
    return pl.pallas_call(
        forecast_kernel,
        out_shape=jax.ShapeDtypeStruct((stream.size // PW, PW), jnp.bfloat16),
        in_specs=[vmem] * 5,
        out_specs=vmem,
        cost_estimate=pl.CostEstimate(
            flops=4 * work,
            bytes_accessed=4 * (stream.size + entry_w.size),
            transcendentals=work // PW,
        ),
        compiler_params=pltpu.CompilerParams(vmem_limit_bytes=2 * VMEM_LIMIT),
        name="forecast",
    )(stream, entry_w, entry_b, exit_w, exit_b)


def residual_kernel(obs_ref, own_ref, prec_ref, resid_ref, misfit_ref):
    patches = prec_ref.shape[0]
    rows = own_ref.shape[0] // patches
    total = jnp.zeros((rows, PW), jnp.float32)
    for p in range(patches):
        part = slice(p * rows, (p + 1) * rows)
        resid = (
            rows_of(obs_ref, p * PW) - own_ref[part, :].astype(jnp.float32)
        ).astype(jnp.bfloat16)
        resid_ref[part, :] = resid
        wide = resid.astype(jnp.float32)
        total = total + wide * wide * prec_ref[p : p + 1, :]
    misfit_ref[...] = jnp.full(misfit_ref.shape, jnp.sum(total))


def residual(obs, own, prec):
    vmem = pl.BlockSpec(memory_space=pltpu.VMEM)
    return pl.pallas_call(
        residual_kernel,
        out_shape=(
            jax.ShapeDtypeStruct(own.shape, jnp.bfloat16),
            jax.ShapeDtypeStruct((SUB, LANES), jnp.float32),
        ),
        in_specs=[vmem] * 3,
        out_specs=(vmem, vmem),
        compiler_params=pltpu.CompilerParams(vmem_limit_bytes=VMEM_LIMIT),
        name="residual",
    )(obs, own, prec)


def terms_kernel(own_ref, far_ref, resid_ref, prec_ref, share_ref, out_ref):
    patches = prec_ref.shape[0]
    rows = own_ref.shape[0] // patches
    members = 2 * rows
    cross = jnp.zeros((members, rows), jnp.float32)
    gram = jnp.zeros((members, members), jnp.float32)
    for p in range(patches):
        part = slice(p * rows, (p + 1) * rows)
        own = own_ref[part, :].astype(jnp.float32)
        far = far_ref[part, :].astype(jnp.float32)
        mean = (jnp.sum(own, axis=0, keepdims=True) + jnp.sum(far, axis=0, keepdims=True)) * (
            1.0 / members
        )
        dev = jnp.concatenate([own - mean, far - mean], axis=0).astype(jnp.bfloat16)
        weighted = (dev.astype(jnp.float32) * prec_ref[p : p + 1, :]).astype(jnp.bfloat16)
        cross = cross + contract(weighted, resid_ref[part, :])
        gram = gram + contract(weighted, dev)
    gram = 0.5 * (gram + gram.T)
    row = lax.broadcasted_iota(jnp.int32, (members, members), 0)
    col = lax.broadcasted_iota(jnp.int32, (members, members), 1)
    gram = gram + jnp.where(row == col, share_ref[0:1, 0:1], 0.0)
    out_ref[...] = jnp.concatenate([cross, jnp.zeros_like(cross), gram], axis=1)


def terms(own, far, resid, prec, share):
    patches = prec.shape[0]
    members = 2 * own.shape[0] // patches
    vmem = pl.BlockSpec(memory_space=pltpu.VMEM)
    return pl.pallas_call(
        terms_kernel,
        out_shape=jax.ShapeDtypeStruct((members, 2 * members), jnp.float32),
        in_specs=[vmem] * 5,
        out_specs=vmem,
        compiler_params=pltpu.CompilerParams(vmem_limit_bytes=VMEM_LIMIT),
        name="terms",
    )(own, far, resid, prec, share)


def terms_plain(own, far, resid, prec, share):
    patches = prec.shape[0]
    rows = own.shape[0] // patches
    members = 2 * rows

    def by_member(value):
        return value.reshape(patches, rows, PW).transpose(1, 0, 2).reshape(rows, patches * PW)

    preds = jnp.concatenate([by_member(own), by_member(far)], axis=0).astype(jnp.float32)
    dev = (preds - jnp.mean(preds, axis=0)).astype(jnp.bfloat16)
    weighted = (dev.astype(jnp.float32) * prec.reshape(-1)).astype(jnp.bfloat16)
    cross = contract(weighted, by_member(resid))
    gram = contract(weighted, dev)
    gram = 0.5 * (gram + gram.T) + share[0, 0] * jnp.eye(members, dtype=jnp.float32)
    return jnp.concatenate([cross, jnp.zeros_like(cross), gram], axis=1)


def eliminate(blocks, first):
    shape = blocks[0].shape
    row = lax.broadcasted_iota(jnp.int32, shape, 0)
    for kb in range(len(blocks)):
        lo = first + kb * SUB
        cols = [
            [jnp.broadcast_to(block[:, lo + j : lo + j + 1], shape) for j in range(SUB)]
            for block in blocks
        ]
        pivot = blocks[kb]
        own = list(cols[kb])
        for p in range(SUB):
            factor = own[p]
            inv = 1.0 / factor[p : p + 1, :]
            line = pivot[p : p + 1, :] * inv
            pivot = jnp.where(row == p, line, pivot - factor * line)
            for j in range(p + 1, SUB):
                line = own[j][p : p + 1, :] * inv
                own[j] = jnp.where(row == p, line, own[j] - factor * line)
        after = []
        for i, block in enumerate(blocks):
            if i == kb:
                after.append(pivot)
                continue
            terms = [cols[i][j] * pivot[j : j + 1, :] for j in range(SUB)]
            while len(terms) > 1:
                terms = [terms[t] + terms[t + 1] for t in range(0, len(terms), 2)]
            after.append(block - terms[0])
        blocks = after
    return blocks


def finish_kernel(scale, shift, mine_ref, other_ref, states_ref, dev_ref, out_ref):
    senders, few, width = out_ref.shape
    rows = senders * few
    members = dev_ref.shape[0]
    row = lax.broadcasted_iota(jnp.int32, (SUB, 2 * members), 0)
    lane = lax.broadcasted_iota(jnp.int32, (SUB, 2 * members), 1)
    blocks = []
    for lo in range(0, members, SUB):
        part = slice(lo, lo + SUB)
        block = (mine_ref[part, :] + other_ref[part, :]) * scale
        blocks.append(block + jnp.where(lane == row + (members + lo), shift, 0.0))
    solved = jnp.concatenate([b[:, :members] for b in eliminate(blocks, members)], axis=0)
    mixing = solved.T[:rows, :].astype(jnp.bfloat16)
    step = min(CHUNK, width)
    for lo in range(0, width, step):
        cols = slice(lo, lo + step)
        move = jnp.dot(mixing, dev_ref[:, cols], preferred_element_type=jnp.float32)
        fresh = states_ref[:, cols].astype(jnp.float32) + move
        for i in range(senders):
            out_ref[i, :, cols] = fresh[i * few : (i + 1) * few, :].astype(jnp.bfloat16)


def finish(scale, shift, few, mine, other, states, dev):
    vmem = pl.BlockSpec(memory_space=pltpu.VMEM)
    return pl.pallas_call(
        lambda *refs: finish_kernel(scale, shift, *refs),
        out_shape=jax.ShapeDtypeStruct(
            (states.shape[0] // few, few, states.shape[1]), jnp.bfloat16
        ),
        in_specs=[vmem] * 4,
        out_specs=vmem,
        compiler_params=pltpu.CompilerParams(vmem_limit_bytes=VMEM_LIMIT),
        name="finish",
    )(mine, other, states, dev)


def finish_plain(scale, shift, few, mine, other, states, dev):
    rows, members = states.shape[0], dev.shape[0]
    joined = (mine + other) * scale
    kmat = joined[:, members:] + shift * jnp.eye(members, dtype=jnp.float32)
    factor = jnp.linalg.cholesky(kmat)
    middle = jax.scipy.linalg.solve_triangular(factor, joined[:, :rows], lower=True)
    solved = jax.scipy.linalg.solve_triangular(factor, middle, lower=True, trans="T")
    mixing = solved.T.astype(jnp.bfloat16)
    return (
        states.astype(jnp.float32) + jnp.dot(mixing, dev, preferred_element_type=jnp.float32)
    ).astype(jnp.bfloat16).reshape(rows // few, few, -1)


def body(
    particle_vectors,
    observed,
    precision,
    entry_projection_matrix,
    entry_offsets,
    exit_projection_matrix,
    exit_offsets,
):
    weights = (entry_projection_matrix, entry_offsets, exit_projection_matrix, exit_offsets)
    count = lax.axis_size("mem")
    if lax.axis_size("rep") != 2 or count < 4 or count & (count - 1):
        raise ValueError("unsupported mesh")
    groups = halves(count)
    state_total = particle_vectors.shape[1] * lax.axis_size("rep")
    member_total = particle_vectors.shape[0] * count
    own_states = to_block(particle_vectors, groups)
    far_states = mirror(own_states, groups)
    own_obs = to_block(observed, groups)
    width = own_states.shape[-1]
    rows = member_total // 2
    me = lax.axis_index("mem")
    place = jnp.where(me < count // 2, me, jnp.bitwise_xor(me - count // 2, count // 4))
    prec_block = lax.dynamic_slice_in_dim(precision, place * width, width).reshape(-1, PW)

    own_preds = forecast(own_states, *weights)
    resid, misfit = residual(own_obs, own_preds, prec_block)
    far_misfit = mirror(misfit, groups)
    far_preds = forecast(far_states, *weights)
    share = (misfit + far_misfit) * (1.0 / member_total)

    small = member_total <= LANES // 2 and member_total % (2 * SUB) == 0
    joined = (terms if small else terms_plain)(own_preds, far_preds, resid, prec_block, share)
    mine, other = total_over_half(joined)

    own_states = own_states.reshape(rows, width)
    far_states = far_states.reshape(rows, width)
    states = jnp.concatenate([own_states, far_states], axis=0).astype(jnp.float32)
    dev = (states - jnp.mean(states, axis=0)).astype(jnp.bfloat16)
    fresh = (finish if small else finish_plain)(
        1.0 / state_total, 1e-06, particle_vectors.shape[0], mine, other, own_states, dev
    )
    back = lax.all_to_all(fresh, "mem", split_axis=0, concat_axis=1, axis_index_groups=groups)
    return back.reshape(particle_vectors.shape)


def solution(mesh):
    placed = (P("mem", "rep"), P("mem", "rep"), P("rep"), P(), P(), P(), P())
    return jax.shard_map(
        body, mesh=mesh, in_specs=placed, out_specs=P("mem", "rep"), check_vma=False
    )
```
